128 devices in a mesh: rep: 1, dp: 128 (over x, y, z, core).
Axes of the slice: x: 4, y: 4, z: 4, core: 2. Of those that a mesh axis runs over, the one named last changes fastest.
Arguments:
- x: bfloat16 [128, 2048, 896], P(('rep', 'dp'))
- dy: bfloat16 [128, 2048, 896], P(('rep', 'dp'))
- w_gate: bfloat16 [2, 896, 2560], P(None, 'dp')
- w_up: bfloat16 [2, 896, 2560], P(None, 'dp')
- w_down: bfloat16 [2, 2560, 896], P(None, 'dp')
Outputs:
- output 1: bfloat16 [128, 2048, 896], P(('rep', 'dp'))
- output 2: bfloat16 [2, 896, 2560], P('rep', 'dp')
- output 3: bfloat16 [2, 896, 2560], P('rep', 'dp')
- output 4: bfloat16 [2, 2560, 896], P('rep', 'dp')
All inputs are finite; a program needn't handle non-finite values.
Results may differ from the reference program's by a relative error of at most 0.018.
Values are sent between devices in bfloat16 or wider.
A program may use at most 1.5 GiB of HBM per device.

```python
import jax
import jax.numpy as jnp
from jax import lax

SEQUENCES = 128
TOKENS = 2048
D = 896
FF = 2560
LAYERS = 2
NAMES = ("w_gate", "w_up", "w_down")
SHAPES = {"w_gate": (LAYERS, D, FF), "w_up": (LAYERS, D, FF), "w_down": (LAYERS, FF, D)}


def bump(key, n, height):
    away = (jnp.arange(n, dtype=jnp.int32) - jax.random.randint(key, (), 0, n, jnp.int32)) % n
    return jnp.where(away < n // 8, height, 1.0)


def together(key, own, strength):
    shared = jax.random.normal(key, own.shape[1:], jnp.float32)
    return (own + strength * shared) * lax.rsqrt(1 + strength * strength)


def setup_inputs(seed: int = 0, part: int = 0) -> dict:
    kx, kdy, ka, kb, kz, kf, kh, kl, *kw = jax.random.split(jax.random.key(seed), 8 + len(NAMES))
    kx, kdy, ka, kb = (jax.random.fold_in(k, part) for k in (kx, kdy, ka, kb))
    shape = (SEQUENCES, TOKENS, D)
    much_x, much_dy = jax.random.uniform(kz, (2,), jnp.float32, 0.0, 1.0)
    layers = 2.0 ** jax.random.uniform(kl, (LAYERS, 1, 1), jnp.float32, -1.0, 1.0)
    x = together(ka, jax.random.normal(kx, shape, jnp.float32), much_x) * bump(kf, D, 4.0)
    dy = together(kb, jax.random.normal(kdy, shape, jnp.float32), much_dy)
    drawn = {"x": x.astype(jnp.bfloat16), "dy": (dy * (SEQUENCES * TOKENS) ** -0.5).astype(jnp.bfloat16)}
    for key, name in zip(kw, NAMES, strict=True):
        w = jax.random.normal(key, SHAPES[name], jnp.float32) * SHAPES[name][1] ** -0.5
        drawn[name] = (w * {"w_gate": 1.0, "w_up": bump(kh, FF, 4.0), "w_down": layers}[name]).astype(jnp.bfloat16)
    return drawn


def matmul(a, w):
    return jnp.dot(a, w, preferred_element_type=jnp.float32).astype(jnp.bfloat16)


def normed(h):
    wide = h.astype(jnp.float32)
    scale = lax.rsqrt(jnp.mean(wide**2, -1, keepdims=True) + 1e-6)
    return (wide * scale).astype(jnp.bfloat16)


def layer(h, w):
    a = normed(h)
    gate = jnp.dot(a, w["w_gate"], preferred_element_type=jnp.float32)
    up = jnp.dot(a, w["w_up"], preferred_element_type=jnp.float32)
    return h + matmul((jax.nn.silu(gate) * up).astype(jnp.bfloat16), w["w_down"])


def stack(weights, h):
    return lax.scan(lambda h, w: (layer(h, w), None), h, weights)[0]


def reference(x, dy, w_gate, w_up, w_down):
    weights = dict(zip(NAMES, (w_gate, w_up, w_down), strict=True))

    def take(so_far, sequence):
        h, by_y = sequence
        _, back = jax.vjp(stack, weights, h)
        by_weights, by_h = back(by_y)
        return jax.tree.map(lambda total, term: total + term.astype(jnp.float32), so_far, by_weights), by_h

    none_yet = {name: jnp.zeros(w.shape, jnp.float32) for name, w in weights.items()}
    by_weights, by_x = lax.scan(take, none_yet, (x, dy))
    return (by_x, *(by_weights[name].astype(jnp.bfloat16) for name in NAMES))
```

```python
import functools
import jax
import jax.numpy as jnp
from jax import lax
from jax.experimental import pallas as pl
from jax.experimental.pallas import tpu as pltpu
from jax.sharding import PartitionSpec as P

STRIDE = (32, 8, 2)
PIECE = ((8, 2560), (8, 2560), (3, 8, 896))
SPLIT = (1280, 1280, 512)


class Place:
    def __init__(self):
        self.me = lax.axis_index("dp")
        self.core = self.me % 2
        self.at = (self.me // 32, self.me // 8 % 4, self.me // 2 % 4)
        self.partner = self.me + 1 - 2 * self.core

    def beside(self, dim, step):
        here = self.at[dim]
        return self.me + ((here + step) % 4 - here) * STRIDE[dim]

    def greet(self):
        barrier = pltpu.get_barrier_semaphore()
        others = [self.beside(d, s) for d in range(3) for s in (1, 3)] + [self.partner]
        for other in others:
            pl.semaphore_signal(barrier, inc=1, device_id={"dp": other}, device_id_type=pl.DeviceIdType.MESH)
        pl.semaphore_wait(barrier, len(others))


def remote(src, dst, send, recv, to):
    return pltpu.make_async_remote_copy(
        src_ref=src, dst_ref=dst, send_sem=send, recv_sem=recv, device_id={"dp": to}, device_id_type=pl.DeviceIdType.MESH)


def lanes(ref, color, half):
    cut = SPLIT[color]
    span = pl.ds(0, cut) if half == 0 else pl.ds(cut, PIECE[color][-1] - cut)
    return ref.at[:, span] if color < 2 else ref.at[:, :, span]


class Gather:
    SEMS = 24

    def __init__(self, place, color, mine, buf, send, recv, local):
        self.o, self.color, self.mine, self.buf, self.send, self.recv, self.local = place, color, mine, buf, send, recv, local
        self.dims = [(color + n) % 3 for n in range(3)]
        self.q = [place.at[d] for d in self.dims]
        self.sent = []

    def group(self, core, s, j, half=None):
        _, p2, p3 = self.q
        if s == 0:
            ref = self.buf.at[core, p3, p2, j]
            return ref if half is None else lanes(ref, self.color, half)
        lead = (core, p3, j) if s == 1 else (core, j)
        return self.buf.at[lead] if half is None else self.buf.at[(*lead, pl.ds(2 * half, 2))]

    def go(self, n, s, j, half, to, core=None):
        ref = self.group(self.o.core if core is None else core, s, j, half)
        copy = remote(ref, ref, self.send.at[n], self.recv.at[n], to)
        copy.start()
        self.sent.append(copy)

    def landed(self, n, s, j, half, core=None):
        ref = self.group(self.o.core if core is None else core, s, j, half)
        remote(ref, ref, self.send.at[n], self.recv.at[n], self.o.partner).wait_recv()

    def own(self):
        copy = pltpu.make_async_copy(self.mine, self.group(self.o.core, 0, self.q[0]), self.local)
        copy.start()
        copy.wait()

    def first(self, s):
        i, right, left = self.q[s], self.o.beside(self.dims[s], 1), self.o.beside(self.dims[s], 3)
        self.go(4 * s, s, i, None, right)
        self.go(4 * s + 1, s, i, None, left)

    def second(self, s):
        i, right, left = self.q[s], self.o.beside(self.dims[s], 1), self.o.beside(self.dims[s], 3)
        self.landed(4 * s, s, (i + 3) % 4, None)
        self.go(4 * s + 2, s, (i + 3) % 4, 0, right)
        self.landed(4 * s + 1, s, (i + 1) % 4, None)
        self.go(4 * s + 3, s, (i + 1) % 4, 1, left)
        b = 12 + 4 * s
        if s == 0:
            return
        self.go(b, s, (i + 3) % 4, None, self.o.partner)
        self.go(b + 1, s, (i + 1) % 4, None, self.o.partner)

    def third(self, s):
        i = self.q[s]
        self.landed(4 * s + 2, s, (i + 2) % 4, 0)
        self.landed(4 * s + 3, s, (i + 2) % 4, 1)
        b = 12 + 4 * s
        if s == 0:
            self.go(b, 1, self.q[1], None, self.o.partner)
        else:
            self.go(b + 2, s, (i + 2) % 4, None, self.o.partner)

    def finish(self):
        other = 1 - self.o.core
        self.landed(12, 1, self.q[1], None, other)
        for s in (1, 2):
            for n, d in enumerate((3, 1, 2)):
                self.landed(12 + 4 * s + n, s, (self.q[s] + d) % 4, None, other)
        for copy in self.sent:
            copy.wait_send()


def gather_kernel(g, u, d, bg, bu, bd, send, recv, local):
    place = Place()
    gathers = [Gather(place, k, m, b, send.at[k], recv.at[k], local.at[k]) for k, (m, b) in enumerate(zip((g, u, d), (bg, bu, bd)))]
    for one in gathers:
        one.own()
    place.greet()
    for s in range(3):
        for one in gathers:
            one.first(s)
        for one in gathers:
            one.second(s)
        for one in gathers:
            one.third(s)
    for one in gathers:
        one.finish()


def all_gather(g, u, d):
    return pl.pallas_call(
        gather_kernel,
        out_shape=[jax.ShapeDtypeStruct((2, 4, 4, 4, *p), jnp.bfloat16) for p in PIECE],
        in_specs=[pl.BlockSpec(memory_space=pl.ANY)] * 3,
        out_specs=[pl.BlockSpec(memory_space=pltpu.VMEM)] * 3,
        scratch_shapes=[pltpu.SemaphoreType.DMA((3, Gather.SEMS)), pltpu.SemaphoreType.DMA((3, Gather.SEMS)), pltpu.SemaphoreType.DMA((3,))],
        compiler_params=pltpu.CompilerParams(collective_id=0, has_side_effects=True, vmem_limit_bytes=60 * 2**20),
    )(g, u, d)


def in_order(color, buf):
    place = {(color + n) % 3: 3 - n for n in range(3)}
    return buf.transpose(place[0], place[1], place[2], 0, *range(4, buf.ndim))


def by_piece(color, rows):
    d = [(color + n) % 3 for n in range(3)]
    return rows.transpose(3, d[2], d[1], d[0], *range(4, rows.ndim))


def pad_blocks(g, u, d):
    return (jnp.pad(g, ((0, 1), (0, 0))), jnp.pad(u, ((0, 1), (0, 0))), jnp.pad(d, ((0, 4), (0, 0))).reshape(3, 8, 896))


class Scatter:
    SEMS = 16

    def __init__(self, place, color, terms, t, r0, r3, r2, r1, out, send, recv, local):
        self.o, self.color, self.terms, self.t, self.r0, self.r, self.out = place, color, terms, t, r0, (r1, r2, r3), out
        self.send, self.recv, self.local = send, recv, local
        self.dims = [(color + n) % 3 for n in range(3)]
        self.q = [place.at[d] for d in self.dims]
        self.sent = []

    def go(self, n, src, dst, to):
        copy = remote(src, dst, self.send.at[n], self.recv.at[n], to)
        copy.start()
        self.sent.append(copy)

    def landed(self, n, dst):
        remote(dst, dst, self.send.at[n], self.recv.at[n], self.o.partner).wait_recv()

    def exchange(self):
        i = self.q[2]
        self.mine = []
        for n, step in enumerate((2, 1, 3, 0)):
            j = (i + step) % 4
            self.go(n, self.terms.at[1 - self.o.core, j], self.r0.at[j], self.o.partner)
            copy = pltpu.make_async_copy(self.terms.at[self.o.core, j], self.t.at[j], self.local.at[n])
            copy.start()
            self.mine.append(copy)

    def add(self, refs, into, pieces):
        def one(p):
            total = refs[0][p].astype(jnp.float32)
            for ref in refs[1:]:
                total += ref[p].astype(jnp.float32)
            into[p] = total.astype(into.dtype)
        pl.loop(0, pieces)(one)

    def flat(self, ref, n):
        return ref

    def add_cores(self, n):
        i = self.q[2]
        j = (i + (2, 1, 3, 0)[n]) % 4
        self.mine[n].wait()
        self.landed(n, self.r0.at[j])
        for a in range(4):
            self.add([self.t.at[j, a], self.r0.at[j, a]], self.t.at[j, a], 4)

    def group(self, s, j, half=None):
        _, p2, p3 = self.q
        if s == 0:
            ref = self.t.at[p3, p2, j]
            return ref if half is None else lanes(ref, self.color, half)
        lead = (p3, j) if s == 1 else (j,)
        return self.t.at[lead] if half is None else self.t.at[(*lead, pl.ds(2 * half, 2))]

    def slot(self, s, n):
        ref = self.r[s].at[n]
        if n >= 2:
            return ref
        return lanes(ref, self.color, n) if s == 0 else ref.at[pl.ds(2 * n, 2)]

    def first(self, s):
        i, right, left = self.q[s], self.o.beside(self.dims[s], 1), self.o.beside(self.dims[s], 3)
        b = 4 + 4 * s
        self.go(b, self.group(s, (i + 2) % 4, 0), self.slot(s, 0), right)
        self.go(b + 1, self.group(s, (i + 2) % 4, 1), self.slot(s, 1), left)

    def second(self, s):
        i, right, left = self.q[s], self.o.beside(self.dims[s], 1), self.o.beside(self.dims[s], 3)
        b = 4 + 4 * s
        for n, j, to in ((0, (i + 1) % 4, right), (1, (i + 3) % 4, left)):
            self.landed(b + n, self.slot(s, n))
            held, came = self.group(s, j, n), self.slot(s, n)
            if s == 2:
                for a in range(2):
                    self.add([held.at[a], came.at[a]], held.at[a], 4)
            elif s == 1:
                self.add([held, came], held, 2)
            else:
                held[...] = (held[...].astype(jnp.float32) + came[...].astype(jnp.float32)).astype(held.dtype)
            self.go(b + 2 + n, self.group(s, j), self.slot(s, 2 + n), to)

    def third(self, s):
        i = self.q[s]
        b = 4 + 4 * s
        for n in (2, 3):
            self.landed(b + n, self.slot(s, n))
        held, one, two = self.group(s, i), self.slot(s, 2), self.slot(s, 3)
        if s == 2:
            for a in range(4):
                self.add([held.at[a], one.at[a], two.at[a]], held.at[a], 4)
        elif s == 1:
            self.add([held, one, two], held, 4)
        else:
            self.out[...] = (held[...].astype(jnp.float32) + one[...].astype(jnp.float32) + two[...].astype(jnp.float32)).astype(self.out.dtype)

    def finish(self):
        for copy in self.sent:
            copy.wait_send()


def scatter_scratch():
    return [[pltpu.VMEM((*lead, *p), jnp.bfloat16) for p in PIECE] for lead in ((4, 4, 4), (4, 4, 4), (4, 4, 4), (4, 4), (4,))]


def scatter_kernel(g, u, d, og, ou, od, ts, r0s, r3s, r2s, r1s, send, recv, local):
    place = Place()
    all_of = [Scatter(place, k, *a, send.at[k], recv.at[k], local.at[k])
              for k, a in enumerate(zip((g, u, d), ts, r0s, r3s, r2s, r1s, (og, ou, od)))]
    place.greet()
    for one in all_of:
        one.exchange()
    for n in range(4):
        for one in all_of:
            one.add_cores(n)
        if n == 0:
            for one in all_of:
                one.first(2)
    for s in (2, 1, 0):
        for one in all_of:
            if s < 2:
                one.first(s)
        for one in all_of:
            one.second(s)
        for one in all_of:
            one.third(s)
    for one in all_of:
        one.finish()


def reduce_scatter(g, u, d):
    return pl.pallas_call(
        scatter_kernel,
        out_shape=[jax.ShapeDtypeStruct(p, jnp.bfloat16) for p in PIECE],
        in_specs=[pl.BlockSpec(memory_space=pl.ANY)] * 3,
        out_specs=[pl.BlockSpec(memory_space=pltpu.VMEM)] * 3,
        scratch_shapes=[*scatter_scratch(), pltpu.SemaphoreType.DMA((3, Scatter.SEMS)), pltpu.SemaphoreType.DMA((3, Scatter.SEMS)),
                        pltpu.SemaphoreType.DMA((3, 4))],
        compiler_params=pltpu.CompilerParams(collective_id=1, has_side_effects=True, vmem_limit_bytes=60 * 2**20),
    )(g, u, d)


NAMES = ("w_gate", "w_up", "w_down")


def matmul(a, w):
    return jnp.dot(a, w, preferred_element_type=jnp.float32).astype(jnp.bfloat16)


def normed(h):
    wide = h.astype(jnp.float32)
    scale = lax.rsqrt(jnp.mean(wide**2, -1, keepdims=True) + 1e-6)
    return (wide * scale).astype(jnp.bfloat16)


def layer(h, w_gate, w_up, w_down):
    a = normed(h)
    gate = jnp.dot(a, w_gate, preferred_element_type=jnp.float32)
    up = jnp.dot(a, w_up, preferred_element_type=jnp.float32)
    return h + matmul((jax.nn.silu(gate) * up).astype(jnp.bfloat16), w_down)


def whole(bufs):
    g, u, d = (in_order(k, b) for k, b in enumerate(bufs))
    return g[..., :7, :].reshape(896, 2560), u[..., :7, :].reshape(896, 2560), d.reshape(128, 24, 896)[:, :20].reshape(2560, 896)


def pieces(g, u, d):
    cut = lambda k, w, rows: by_piece(k, jnp.pad(w.reshape(4, 4, 4, 2, rows, -1), ((0, 0),) * 4 + ((0, -rows % 8), (0, 0))))
    return cut(0, g, 7), cut(1, u, 7), cut(2, d, 20).reshape(2, 4, 4, 4, 3, 8, 896)


def scattered(terms):
    g, u, d = reduce_scatter(*pieces(*terms))
    return g[:7], u[:7], d.reshape(24, 896)[:20]


def solution(mesh):
    def step(x, dy, w_gate, w_up, w_down):
        h, by_h = x[0], dy[0]
        backs = []
        for n in range(2):
            w = whole(all_gather(*pad_blocks(w_gate[n], w_up[n], w_down[n])))
            h, back = jax.vjp(layer, h, *w)
            backs.append(back)
        sums = [None, None]
        for n in (1, 0):
            by_h, *terms = backs[n](by_h)
            sums[n] = scattered(terms)
        return (by_h[None], *(jnp.stack([sums[0][k], sums[1][k]]) for k in range(3)))

    rows = P(("rep", "dp"))
    weights = [P(None, "dp")] * 3
    return jax.shard_map(step, mesh=mesh, in_specs=(rows, rows, *weights), out_specs=(rows, *weights), check_vma=False)
```

```python
import math

import jax
import jax.numpy as jnp
from jax import lax
from jax.experimental import pallas as pl
from jax.experimental.pallas import tpu as pltpu
from jax.sharding import PartitionSpec as P

BF16, F32 = jnp.bfloat16, jnp.float32
D, FF, TOKENS = 896, 2560, 2048
STRIDE = (32, 8, 2)
WIDTHS = ((1024, 768, 768), (768, 1024, 768), (896, 896, 896))
UNITS = [(m, c, c if m == 2 else sum(some[:c]), w) for m, some in enumerate(WIDTHS) for c, w in enumerate(some)]
AFTER, OVER, BEFORE = 1, 2, 3
TORUS = (4, 4, 4)
EDGE = pl.ds(0, 4)
ARRIVE = (BEFORE, AFTER, OVER)


def cut(refs, *sizes):
    refs = list(refs)
    return *[[refs.pop(0) for _ in range(size)] for size in sizes], refs


class Place:
    def __init__(self):
        self.me = lax.axis_index("dp")
        self.core = self.me % 2
        self.at = (self.me // 32, self.me // 8 % 4, self.me // 2 % 4)
        self.partner = self.me + 1 - 2 * self.core

    def beside(self, dim, step):
        here = self.at[dim]
        return self.me + ((here + step) % 4 - here) * STRIDE[dim]

    def greet(self):
        barrier = pltpu.get_barrier_semaphore()
        others = [self.beside(d, s) for d in range(3) for s in (AFTER, BEFORE)] + [self.partner]
        for other in others:
            pl.semaphore_signal(barrier, inc=1, device_id={"dp": other}, device_id_type=pl.DeviceIdType.MESH)
        pl.semaphore_wait(barrier, len(others))


class Ring:
    def __init__(self, place, color, width, send, recv):
        self.o, self.width, self.send, self.recv = place, width, send, recv
        self.dims = [(color + n) % 3 for n in range(3)]
        self.q = [place.at[d] for d in self.dims]

    def copy(self, n, src, dst, to):
        return pltpu.make_async_remote_copy(
            src_ref=src, dst_ref=dst, send_sem=self.send.at[n], recv_sem=self.recv.at[n],
            device_id={"dp": to}, device_id_type=pl.DeviceIdType.MESH)

    def go(self, n, src, dst, to):
        self.copy(n, src, dst, to).start()

    def landed(self, n, dst):
        self.copy(n, dst, dst, self.o.partner).wait_recv()

    def sent(self, n, ref):
        self.copy(n, ref, ref, self.o.partner).wait_send()

    def index(self, s, j, half=None):
        at = [None] * 3
        for n, d in enumerate(self.dims):
            at[d] = EDGE if n < s else j if n == s else self.q[n]
        if half is not None and s:
            at[self.dims[s - 1]] = pl.ds(2 * half, 2)
        return tuple(at)

    def lanes(self, half):
        cut = 512
        return pl.ds(0, cut) if half == 0 else pl.ds(cut, self.width - cut)

    def turn(self, s, step):
        return (self.q[s] + step) % 4

    def sides(self, s):
        return self.q[s], self.o.beside(self.dims[s], AFTER), self.o.beside(self.dims[s], BEFORE)


class Gather(Ring):
    SEMS = 19

    def __init__(self, place, color, width, mine, buf, send, recv, local):
        super().__init__(place, color, width, send, recv)
        self.mine, self.buf, self.local = mine, buf, local

    def group(self, core, s, j, half=None):
        ref = self.buf.at[(*self.index(s, j, half), core)]
        return ref.at[:, self.lanes(half)] if half is not None and s == 0 else ref

    def pass_on(self, n, s, j, half, to):
        ref = self.group(self.o.core, s, j, half)
        self.go(n, ref, ref, to)

    def came(self, n, s, j, half=None, core=None):
        self.landed(n, self.group(self.o.core if core is None else core, s, j, half))

    def load(self):
        pltpu.make_async_copy(self.mine, self.group(self.o.core, 0, self.q[0]), self.local).start()

    def loaded(self):
        pltpu.make_async_copy(self.mine, self.group(self.o.core, 0, self.q[0]), self.local).wait()

    def first(self, s):
        i, right, left = self.sides(s)
        self.pass_on(4 * s, s, i, None, right)
        self.pass_on(4 * s + 1, s, i, None, left)

    def second(self, s):
        i, right, left = self.sides(s)
        self.came(4 * s, s, self.turn(s, BEFORE))
        self.pass_on(4 * s + 2, s, self.turn(s, BEFORE), 0, right)
        self.came(4 * s + 1, s, self.turn(s, AFTER))
        self.pass_on(4 * s + 3, s, self.turn(s, AFTER), 1, left)
        if s:
            b = 10 + 3 * s
            self.pass_on(b, s, self.turn(s, BEFORE), None, self.o.partner)
            self.pass_on(b + 1, s, self.turn(s, AFTER), None, self.o.partner)

    def third(self, s):
        i = self.q[s]
        self.came(4 * s + 2, s, self.turn(s, OVER), 0)
        self.came(4 * s + 3, s, self.turn(s, OVER), 1)
        if s == 0:
            self.pass_on(12, 1, self.q[1], None, self.o.partner)
        else:
            self.pass_on(12 + 3 * s, s, self.turn(s, OVER), None, self.o.partner)

    def finish(self):
        other = 1 - self.o.core
        self.came(12, 1, self.q[1], core=other)
        for s in (1, 2):
            for m, step in enumerate(ARRIVE):
                self.came(10 + 3 * s + m, s, self.turn(s, step), core=other)

    def closed(self):
        for s, i in enumerate(self.q):
            for m, (step, half) in enumerate(((0, None), (0, None), (3, 0), (1, 1))):
                self.sent(4 * s + m, self.group(self.o.core, s, self.turn(s, step), half))
            for m, step in enumerate(ARRIVE if s else ()):
                self.sent(10 + 3 * s + m, self.group(self.o.core, s, self.turn(s, step)))
        self.sent(12, self.group(self.o.core, 1, self.q[1]))


class Scatter(Ring):
    SEMS = 16

    def __init__(self, place, color, width, terms, r0, r3, r2, r1, out, send, recv):
        super().__init__(place, color, width, send, recv)
        self.terms, self.r0, self.r, self.out = terms, r0, (r1, r2, r3), out

    def order(self, n):
        return (self.q[2] + (2, 1, 3, 0)[n]) % 4

    def exchange(self):
        for n in range(4):
            at = self.index(2, self.order(n))
            self.go(n, self.terms.at[(*at, 1 - self.o.core)], self.r0.at[at], self.o.partner)

    def group(self, s, j, half=None):
        ref = self.terms.at[(*self.index(s, j, half), self.o.core)]
        return ref.at[:, self.lanes(half)] if half is not None and s == 0 else ref

    def slot(self, s, n):
        if n >= 2:
            return self.r[s].at[n - 1]
        ref = self.r[s].at[0]
        if s == 0:
            return ref.at[:, self.lanes(n)]
        at = [EDGE] * s
        at[sorted(self.dims[:s]).index(self.dims[s - 1])] = pl.ds(2 * n, 2)
        return ref.at[tuple(at)]

    def add(self, held, others):
        lead = held.shape[:-2]
        if not lead:
            held[...] = sum((o[...].astype(F32) for o in others), held[...].astype(F32)).astype(BF16)
            return

        def one(p):
            at = (p,) if len(lead) == 1 else (p // lead[1], p % lead[1])
            held[at] = sum((o[at].astype(F32) for o in others), held[at].astype(F32)).astype(BF16)

        pl.loop(0, math.prod(lead), unroll=2 if len(lead) == 1 else 4)(one)

    def add_cores(self, n):
        at = self.index(2, self.order(n))
        self.landed(n, self.r0.at[at])
        self.add(self.terms.at[(*at, self.o.core)], [self.r0.at[at]])

    def first(self, s):
        i, right, left = self.sides(s)
        b = 4 + 4 * s
        self.go(b, self.group(s, self.turn(s, OVER), 0), self.slot(s, 0), right)
        self.go(b + 1, self.group(s, self.turn(s, OVER), 1), self.slot(s, 1), left)

    def second(self, s):
        i, right, left = self.sides(s)
        b = 4 + 4 * s
        for n, j, to in ((0, self.turn(s, AFTER), right), (1, self.turn(s, BEFORE), left)):
            self.landed(b + n, self.slot(s, n))
            self.add(self.group(s, j, n), [self.slot(s, n)])
            self.go(b + 2 + n, self.group(s, j), self.slot(s, 2 + n), to)

    def closed(self):
        for n in range(4):
            self.sent(n, self.terms.at[(*self.index(2, self.order(n)), self.o.core)])
        for s, i in enumerate(self.q):
            for m, (step, half) in enumerate(((2, 0), (2, 1), (1, None), (3, None))):
                self.sent(4 + 4 * s + m, self.group(s, self.turn(s, step), half))

    def third(self, s):
        b = 4 + 4 * s
        for n in (2, 3):
            self.landed(b + n, self.slot(s, n))
        held, others = self.group(s, self.q[s]), [self.slot(s, 2), self.slot(s, 3)]
        if s:
            self.add(held, others)
        else:
            self.out[...] = sum((o[...].astype(F32) for o in others), held[...].astype(F32)).astype(BF16)


def block_of(refs, matrix, start, width):
    return refs[matrix].at[start] if matrix == 2 else refs[matrix].at[:, pl.ds(start, width)]


def gathers_of(place, blocks, bufs, send, recv, local):
    return [Gather(place, c, w, block_of(blocks, m, at, w), bufs[n], send.at[n], recv.at[n], local.at[n])
            for n, (m, c, at, w) in enumerate(UNITS)]


def scatters_of(place, terms, r0s, r3s, r2s, r1s, outs, send, recv):
    return [Scatter(place, c, w, terms[n], r0s[n], r3s[n], r2s[n], r1s[n], block_of(outs, m, at, w), send.at[n], recv.at[n])
            for n, (m, c, at, w) in enumerate(UNITS)]


def unit_arrays(*lead):
    return [(*lead, 8, w) for _, _, _, w in UNITS]


def pick(rows, cols, back):
    r = lax.broadcasted_iota(jnp.int32, (rows, cols), 1 if back else 0)
    c = lax.broadcasted_iota(jnp.int32, (rows, cols), 0 if back else 1)
    return ((r == 7 * (c >> 3) + (c & 7)) & ((c & 7) < 7)).astype(F32).astype(BF16)


def dot(a, b, dims=((1,), (0,))):
    return lax.dot_general(a, b, (dims, ((), ())), preferred_element_type=F32)


def unpad(unit, buf, w, wide):
    matrix, _, start, width = UNITS[unit]
    for x in range(4):
        rows = buf[x].astype(F32).reshape(256, width).astype(BF16)
        w[pl.ds(224 * x, 224), pl.ds(start, width)] = dot(wide[...], rows).astype(BF16)


def unpad_down(bufs, w, tall):
    def some(x):
        for i in range(32):
            for r in range(3):
                tall[pl.ds(20 * i + 8 * r, 8), :] = bufs[r][x, i // 8, i // 2 % 4, i % 2].astype(F32)
        w[pl.ds(pl.multiple_of(640 * x, 128), 640), :] = tall[0:640, :].astype(BF16)
    pl.loop(0, 4)(some)

TILE, PART = 512, 1280
TILES, PARTS = TOKENS // TILE, FF // PART
FEW = 512
HERE, VM = pl.BlockSpec(memory_space=pl.ANY), pl.BlockSpec(memory_space=pltpu.VMEM)


def normed(h):
    wide = h.astype(F32)
    scale = lax.rsqrt(jnp.mean(wide**2, -1, keepdims=True) + 1e-6)
    return wide, scale


def gather_semaphores():
    return [pltpu.SemaphoreType.DMA((9, Gather.SEMS)), pltpu.SemaphoreType.DMA((9, Gather.SEMS)), pltpu.SemaphoreType.DMA((9,))]


def up_kernel(x, *refs):
    blocks0, blocks1, (h1, a_out, gate_out, up_out), kept, bufs1, bufs0, w, refs = cut(refs, 3, 3, 4, 3, 9, 9, 3)
    tall, wide, a, act, send0, recv0, local0, send1, recv1, local1, keep = refs
    keeps = [pltpu.make_async_copy(f, t, keep.at[m]) for m, (f, t) in enumerate(zip((*w, a), (*kept, a_out)))]
    rows, part = tiled(TILE, PART)

    def units():
        place = Place()
        return [*gathers_of(place, blocks0, bufs0, send0, recv0, local0), *gathers_of(place, blocks1, bufs1, send1, recv1, local1)]

    def steps(plan, all_of):
        for what, which in zip(plan[::2], plan[1::2]):
            some = [k for k, unit in zip(all_of, "ggguuuddd" + "l" * 9) if unit == which]
            if what == "a":
                for k in some:
                    k.loaded()
                    k.first(0)
                continue
            s = "bdf".find(what) if what in "bdf" else "ceg".find(what)
            for k in some:
                if what in "bdf":
                    k.second(s)
                else:
                    k.third(s)
                    if s < 2:
                        k.first(s + 1)

    def beside(step, plans):
        for n, plan in enumerate(plans):
            if plan:
                pl.when(step == n)(lambda: steps(plan, units()))

    def lanes_of(j):
        return pl.ds(pl.multiple_of(j * PART, PART), PART)

    def rows_of(i):
        return pl.ds(pl.multiple_of(i * TILE, TILE), TILE)

    def ready(matrix):
        for k in first[3 * matrix:3 * matrix + 3]:
            k.finish()
        if matrix == 2:
            unpad_down(bufs0[6:], w[2], tall)
        else:
            for n in range(3 * matrix, 3 * matrix + 3):
                unpad(n, bufs0[n], w[matrix], wide)
        keeps[matrix].start()

    first = units()
    for k in first:
        k.load()
    first[0].o.greet()
    wide[...] = pick(224, 256, False)
    steps("agauad" "bgcgbucudgegbdcddudd" "fgeuedgg", first)
    ready(0)
    steps("fu", first)

    def gate_body(h, out):
        i, j = pl.program_id(0), pl.program_id(1)

        @pl.when(j == 0)
        def _():
            wide_h, scale = normed(h[...])
            a[rows_of(i), :] = (wide_h * scale).astype(BF16)

        beside(i * PARTS + j, ("al", "", "bl", "clfd", "gu", "dl", "el", ""))
        out[...] = dot(a[rows_of(i), :], w[0][:, lanes_of(j)])

    pltpu.emit_pipeline(gate_body, grid=(TILES, PARTS), in_specs=[rows], out_specs=[part])(x, gate_out)
    keeps[3].start()
    ready(1)
    steps("gd", first)

    def up_body(gate, out):
        i, j = pl.program_id(0), pl.program_id(1)
        beside(i * PARTS + j, ("", "", "", "", "", "", "", "fl"))
        up = dot(a[rows_of(i), :], w[1][:, lanes_of(j)])
        out[...] = up
        act[rows_of(i), lanes_of(j)] = (gate[...] * jax.nn.sigmoid(gate[...]) * up).astype(BF16)

    pltpu.emit_pipeline(up_body, grid=(TILES, PARTS), in_specs=[part], out_specs=[part])(gate_out, up_out)
    ready(2)

    def down_body(h, out):
        i = pl.program_id(0)
        beside(i, ("", "", "gl"))
        down = dot(act[rows_of(i), :], w[2][...]).astype(BF16)
        out[...] = (h[...].astype(F32) + down.astype(F32)).astype(BF16)

    tile = pl.BlockSpec((TILE, D), lambda i: (i, 0))
    pltpu.emit_pipeline(down_body, grid=(TILES,), in_specs=[tile], out_specs=[tile])(x, h1)
    for k in first[9:]:
        k.finish()
    for k in first:
        k.closed()
    for k in keeps:
        k.wait()


def params(collective=None):
    return pltpu.CompilerParams(collective_id=collective, has_side_effects=collective is not None, vmem_limit_bytes=67043328)


def tiled(tile, part):
    return pl.BlockSpec((tile, D), lambda i, j: (i, 0)), pl.BlockSpec((tile, part), lambda i, j: (i, j))


def like(shape, dtype=BF16):
    return jax.ShapeDtypeStruct(shape, dtype)


WEIGHTS = ((D, FF), (D, FF), (FF, D))
STATES, HIDDEN = (TOKENS, D), (TOKENS, FF)


def forward(x, blocks0, blocks1):
    units = unit_arrays(*TORUS, 2)
    out = pl.pallas_call(
        up_kernel,
        out_shape=[like(STATES), like(STATES), like(HIDDEN, F32), like(HIDDEN, F32), *map(like, WEIGHTS), *map(like, units)],
        in_specs=[HERE] * 7,
        out_specs=[HERE] * 16,
        scratch_shapes=[
            *[pltpu.VMEM(s, BF16) for s in (*units, *WEIGHTS)],
            pltpu.VMEM((648, D), F32), pltpu.VMEM((224, 256), BF16), pltpu.VMEM(STATES, BF16), pltpu.VMEM(HIDDEN, BF16),
            *gather_semaphores(), *gather_semaphores(), pltpu.SemaphoreType.DMA((4,))],
        compiler_params=params(0),
    )(x, *blocks0, *blocks1)
    return cut(out, *[1] * 4, 3)


def hidden_back(gate, up, by_act):
    sig = jax.nn.sigmoid(gate)
    silu = gate * sig
    by_silu = by_act * up
    by_gate = by_silu * (sig + silu * (1 - sig))
    return (silu * up).astype(BF16), by_gate.astype(BF16), (by_act * silu).astype(BF16)


def norm_back(h, by_h, by_gate_a, by_up_a):
    by_a = (by_gate_a.astype(BF16).astype(F32) + by_up_a.astype(BF16).astype(F32)).astype(BF16).astype(F32)
    wide, scale = normed(h)
    by_scale = jnp.sum(by_a * wide, -1, keepdims=True)
    by_wide = by_a * scale - wide * (by_scale * scale**3 / D)
    return (by_h.astype(F32) + by_wide.astype(BF16).astype(F32)).astype(BF16)


BACK = ((1,), (1,))


def back_part(h, by_h, gate, up, w, lanes, outs, by_in, accs, last):
    by_act = dot(by_h[...], w[2][lanes, :], BACK).astype(BF16).astype(F32)
    for out, value in zip(outs, hidden_back(gate, up, by_act)):
        out[...] = value
    for k, acc in enumerate(accs):
        acc[...] += dot(outs[k + 1][...], w[k][:, lanes], BACK)

    @pl.when(last)
    def _():
        by_in[...] = norm_back(h[...], by_h[...], accs[0][...], accs[1][...])


def top_kernel(*refs):
    bufs, (h, by_h, a), outs, (by_in,), w, accs, (stage, tall, wide, fetch) = cut(refs, 9, 3, 3, 1, 3, 2)
    i, j = pl.program_id(0), pl.program_id(1)

    @pl.when((i == 0) & (j == 0))
    def _():
        held = [stage.at[n % 3, :, :, :, :, :, pl.ds(0, UNITS[n][3])] for n in range(9)]
        copies = [pltpu.make_async_copy(bufs[n], held[n], fetch.at[n % 3]) for n in range(9)]
        for n in range(3):
            copies[n].start()
        wide[...] = pick(224, 256, False)
        for n in range(6):
            copies[n].wait()
            unpad(n, held[n], w[n // 3], wide)
            copies[n + 3].start()
        for n in range(6, 9):
            copies[n].wait()
        unpad_down(held[6:], w[2], tall)

    @pl.when(j == 0)
    def _():
        wide_h, scale = normed(h[...])
        a[...] = (wide_h * scale).astype(BF16)
        for acc in accs:
            acc[...] = jnp.zeros_like(acc)

    lanes = pl.ds(pl.multiple_of(j * PART, PART), PART)
    gate = dot(a[...], w[0][:, lanes])
    up = dot(a[...], w[1][:, lanes])
    back_part(h, by_h, gate, up, w, lanes, outs, by_in, accs, j == PARTS - 1)


def top(h, by_h, bufs):
    rows, part = tiled(TILE, PART)
    return pl.pallas_call(
        top_kernel,
        grid=(TILES, PARTS),
        out_shape=[like(STATES), *[like(HIDDEN)] * 3, like(STATES)],
        in_specs=[*[HERE] * 9, rows, rows],
        out_specs=[rows, part, part, part, rows],
        scratch_shapes=[*[pltpu.VMEM(s, BF16) for s in WEIGHTS], *[pltpu.VMEM((TILE, D), F32)] * 2,
                        pltpu.VMEM((3, 4, 4, 4, 2, 8, 1024), BF16), pltpu.VMEM((648, D), F32), pltpu.VMEM((224, 256), BF16),
                        pltpu.SemaphoreType.DMA((3,))],
        compiler_params=params(),
    )(*bufs, h, by_h)


COLS = 256


def sum_kernel(below, *refs):
    (a, by_h, act, by_gate, by_up), came, outs, gone, refs = cut(refs, 5, 7 * below, 3, 4 * below)
    terms, r0s, r3s, r2s, r1s, refs = cut(refs, *[len(UNITS)] * 5)
    back, send, recv, fetch, fetch_wide, whole = refs
    def all_units():
        return scatters_of(Place(), terms, r0s, r3s, r2s, r1s, outs, send, recv)

    units = all_units()

    def cores(some):
        for n in range(4):
            for k in some:
                k.add_cores(n)
            if not n:
                for k in some:
                    k.first(2)

    def steps(plan, units=units):
        for what, which in zip(plan[::2], plan[1::2]):
            some = [k for k, unit in zip(units, "ggguuuddd") if unit == which]
            if what == "c":
                cores(some)
            for k in some:
                if what == "b":
                    k.second(2)
                elif what == "f":
                    k.third(2)
                    k.first(1)
                elif what == "h":
                    k.second(1)
                elif what == "k":
                    k.third(1)
                    k.first(0)
                elif what == "m":
                    k.second(0)
                elif what == "p":
                    k.third(0)

    units[0].o.greet()
    back[...] = pick(256, 224, True)

    def make_all(side, tall, cols, made):
        def wide_copy(x):
            return pltpu.make_async_copy(act.at[:, pl.ds(pl.multiple_of(640 * x, 128), 640)], cols.at[x % 2], fetch_wide.at[x % 2])

        def copy(src, t):
            return pltpu.make_async_copy(
                src.at[:, pl.ds(pl.multiple_of(COLS * t, COLS), COLS)], cols.at[t % 2, :, pl.ds(0, COLS)], fetch.at[t % 2])

        states = pltpu.make_async_copy(by_h, side, whole)
        states.start()
        wide_copy(0).start()
        states.wait()
        tall[640:648, :] = jnp.zeros((8, D), F32)

        def down(x):
            wide_copy(x).wait()
            pl.when(x < 3)(lambda: wide_copy(x + 1).start())
            tall[0:640, :] = dot(cols[x % 2], side[...], ACROSS)
            for i in range(32):
                for r in range(3):
                    terms[6 + r][x, i // 8, i // 2 % 4, i % 2] = tall[pl.ds(20 * i + 8 * r, 8), :].astype(BF16)

        pl.loop(0, 4)(down)
        states = pltpu.make_async_copy(a, side, whole)
        states.start()
        copy(by_gate, 0).start()
        for k in units[6:]:
            k.exchange()
        states.wait()

        for unit, then in enumerate(("cd", "", "bdcg", "fd", "hdbg", "kdfg")):
            matrix, _, start, width = UNITS[unit]
            src, term = (by_gate, by_up)[matrix], terms[unit]

            def one(n):
                t = start // COLS + n
                copy(src, t).wait()
                pl.when(t < FF // COLS - 1)(lambda: copy(src, t + 1).start())
                lanes = pl.ds(pl.multiple_of(n * COLS, COLS), COLS)
                made[:, lanes] = dot(side[...], cols[t % 2, :, 0:COLS], ACROSS).astype(BF16)

            pl.loop(0, width // COLS)(one)
            for x in range(4):
                term[x] = dot(back[...], made[224 * x:224 * (x + 1), 0:width]).reshape(4, 4, 2, 8, width).astype(BF16)
            if unit == 2:
                copy(by_up, 0).start()
            units[unit].exchange()
            steps(then)

    pl.run_scoped(make_all, pltpu.VMEM(STATES, BF16), pltpu.VMEM((648, D), F32), pltpu.VMEM((2, TOKENS, 640), BF16),
                  pltpu.VMEM((D, 1024), BF16))

    if not below:
        steps("mdcuhgpdkgbumgfupghukumupu")
    else:
        def lower(*refs):
            w, accs = cut(refs, 3)
            loads = [pltpu.make_async_copy(came[k + 4], w[k], fetch.at[0] if not k else fetch_wide.at[k - 1]) for k in range(3)]
            for load in loads:
                load.start()
            steps("mdcu")
            for load in loads:
                load.wait()
            rows, part = tiled(TILE, FEW)
            once = pl.BlockSpec(rows.block_shape, rows.index_map, pipeline_mode=pl.Buffered(1))

            def body(h, by_next, gate, up, act_out, by_gate_out, by_up_out, by_in):
                i, j = pl.program_id(0), pl.program_id(1)
                for n, plan in enumerate(("hgpd", "", "kg", "bu", "mg", "", "pg", "fu", "", "hu", "", "ku", "", "mu", "", "pu")):
                    if plan:
                        pl.when(i * (FF // FEW) + j == n)(lambda: steps(plan, all_units()))

                @pl.when(j == 0)
                def _():
                    for acc in accs:
                        acc[...] = jnp.zeros_like(acc)

                lanes = pl.ds(pl.multiple_of(j * FEW, FEW), FEW)
                back_part(h, by_next, gate[...], up[...], w, lanes, (act_out, by_gate_out, by_up_out), by_in, accs, j == FF // FEW - 1)

            pltpu.emit_pipeline(
                body, grid=(TILES, FF // FEW), in_specs=[once, once, part, part], out_specs=[part, part, part, rows])(*came[:4], *gone)

        pl.run_scoped(lower, *[pltpu.VMEM(s, BF16) for s in WEIGHTS], *[pltpu.VMEM((TILE, D), F32)] * 2)
    for k in units:
        k.closed()


ACROSS = ((0,), (0,))


def summed(a, by_h, act, by_gate, by_up, below=()):
    arrays = lambda *lead: [pltpu.VMEM(s, BF16) for s in unit_arrays(*lead)]
    more = [*[like(HIDDEN)] * 3, like(STATES)] if below else []
    g, u, d, *gone = pl.pallas_call(
        lambda *refs: sum_kernel(bool(below), *refs),
        out_shape=[like((8, FF)), like((8, FF)), like((3, 8, D)), *more],
        in_specs=[HERE] * (5 + len(below)),
        out_specs=[VM] * 3 + [HERE] * len(more),
        scratch_shapes=[
            *arrays(*TORUS, 2), *arrays(*TORUS), *arrays(3, 4, 4), *arrays(3, 4), *arrays(3),
            pltpu.VMEM((256, 224), BF16),
            pltpu.SemaphoreType.DMA((9, Scatter.SEMS)), pltpu.SemaphoreType.DMA((9, Scatter.SEMS)),
            pltpu.SemaphoreType.DMA((2,)), pltpu.SemaphoreType.DMA((2,)), pltpu.SemaphoreType.DMA],
        compiler_params=params(1 + len(below)),
    )(a, by_h, act, by_gate, by_up, *below)
    return (g[:7], u[:7], d.reshape(24, D)[:20]), gone


def pad_blocks(g, u, d):
    return jnp.pad(g, ((0, 1), (0, 0))), jnp.pad(u, ((0, 1), (0, 0))), jnp.pad(d, ((0, 4), (0, 0))).reshape(3, 8, D)


def solution(mesh):
    def step(x, dy, w_gate, w_up, w_down):
        x, dy = x[0], dy[0]
        blocks = [pad_blocks(w_gate[n], w_up[n], w_down[n]) for n in range(2)]
        (h1,), (a0,), (gate,), (up,), w0, bufs1 = forward(x, *blocks)
        a1, act1, by_gate1, by_up1, by_h1 = top(h1, dy, bufs1)
        sums1, (*parts0, by_x) = summed(a1, dy, act1, by_gate1, by_up1, below=(x, by_h1, gate, up, *w0))
        sums0, _ = summed(a0, by_h1, *parts0)
        return (by_x[None], *(jnp.stack([sums0[k], sums1[k]]) for k in range(3)))

    rows = P(("rep", "dp"))
    weights = [P(None, "dp")] * 3
    return jax.shard_map(step, mesh=mesh, in_specs=(rows, rows, *weights), out_specs=(rows, *weights), check_vma=False)
```

```python
import math

import jax
import jax.numpy as jnp
from jax import lax
from jax.experimental import pallas as pl
from jax.experimental.pallas import tpu as pltpu
from jax.sharding import PartitionSpec as P

BF16, F32 = jnp.bfloat16, jnp.float32
D, FF, TOKENS = 896, 2560, 2048
STRIDE = (32, 8, 2)
WIDTHS = ((1024, 768, 768), (768, 1024, 768), (896, 896, 896))
UNITS = [(m, c, c if m == 2 else sum(some[:c]), w) for m, some in enumerate(WIDTHS) for c, w in enumerate(some)]
AFTER, OVER, BEFORE = 1, 2, 3
TORUS = (4, 4, 4)
EDGE = pl.ds(0, 4)
ARRIVE = (BEFORE, AFTER, OVER)


def cut(refs, *sizes):
    refs = list(refs)
    return *[[refs.pop(0) for _ in range(size)] for size in sizes], refs


class Place:
    def __init__(self):
        self.me = lax.axis_index("dp")
        self.core = self.me % 2
        self.at = (self.me // 32, self.me // 8 % 4, self.me // 2 % 4)
        self.partner = self.me + 1 - 2 * self.core

    def beside(self, dim, step):
        here = self.at[dim]
        return self.me + ((here + step) % 4 - here) * STRIDE[dim]

    def greet(self):
        barrier = pltpu.get_barrier_semaphore()
        others = [self.beside(d, s) for d in range(3) for s in (AFTER, BEFORE)] + [self.partner]
        for other in others:
            pl.semaphore_signal(barrier, inc=1, device_id={"dp": other}, device_id_type=pl.DeviceIdType.MESH)
        pl.semaphore_wait(barrier, len(others))


class Ring:
    def __init__(self, place, color, width, send, recv):
        self.o, self.width, self.send, self.recv = place, width, send, recv
        self.dims = [(color + n) % 3 for n in range(3)]
        self.q = [place.at[d] for d in self.dims]

    def copy(self, n, src, dst, to):
        return pltpu.make_async_remote_copy(
            src_ref=src, dst_ref=dst, send_sem=self.send.at[n], recv_sem=self.recv.at[n],
            device_id={"dp": to}, device_id_type=pl.DeviceIdType.MESH)

    def go(self, n, src, dst, to):
        self.copy(n, src, dst, to).start()

    def landed(self, n, dst):
        self.copy(n, dst, dst, self.o.partner).wait_recv()

    def sent(self, n, ref):
        self.copy(n, ref, ref, self.o.partner).wait_send()

    def index(self, s, j, half=None):
        at = [None] * 3
        for n, d in enumerate(self.dims):
            at[d] = EDGE if n < s else j if n == s else self.q[n]
        if half is not None and s:
            at[self.dims[s - 1]] = pl.ds(2 * half, 2)
        return tuple(at)

    def lanes(self, half):
        cut = 512
        return pl.ds(0, cut) if half == 0 else pl.ds(cut, self.width - cut)

    def turn(self, s, step):
        return (self.q[s] + step) % 4

    def sides(self, s):
        return self.q[s], self.o.beside(self.dims[s], AFTER), self.o.beside(self.dims[s], BEFORE)


class Gather(Ring):
    SEMS = 19

    def __init__(self, place, color, width, mine, buf, send, recv, local):
        super().__init__(place, color, width, send, recv)
        self.mine, self.buf, self.local = mine, buf, local

    def group(self, core, s, j, half=None):
        ref = self.buf.at[(*self.index(s, j, half), core)]
        return ref.at[:, self.lanes(half)] if half is not None and s == 0 else ref

    def pass_on(self, n, s, j, half, to):
        ref = self.group(self.o.core, s, j, half)
        self.go(n, ref, ref, to)

    def came(self, n, s, j, half=None, core=None):
        self.landed(n, self.group(self.o.core if core is None else core, s, j, half))

    def load(self):
        pltpu.make_async_copy(self.mine, self.group(self.o.core, 0, self.q[0]), self.local).start()

    def loaded(self):
        pltpu.make_async_copy(self.mine, self.group(self.o.core, 0, self.q[0]), self.local).wait()

    def first(self, s):
        i, right, left = self.sides(s)
        self.pass_on(4 * s, s, i, None, right)
        self.pass_on(4 * s + 1, s, i, None, left)

    def second(self, s):
        i, right, left = self.sides(s)
        self.came(4 * s, s, self.turn(s, BEFORE))
        self.pass_on(4 * s + 2, s, self.turn(s, BEFORE), 0, right)
        self.came(4 * s + 1, s, self.turn(s, AFTER))
        self.pass_on(4 * s + 3, s, self.turn(s, AFTER), 1, left)
        if s:
            b = 10 + 3 * s
            self.pass_on(b, s, self.turn(s, BEFORE), None, self.o.partner)
            self.pass_on(b + 1, s, self.turn(s, AFTER), None, self.o.partner)

    def third(self, s):
        i = self.q[s]
        self.came(4 * s + 2, s, self.turn(s, OVER), 0)
        self.came(4 * s + 3, s, self.turn(s, OVER), 1)
        if s == 0:
            self.pass_on(12, 1, self.q[1], None, self.o.partner)
        else:
            self.pass_on(12 + 3 * s, s, self.turn(s, OVER), None, self.o.partner)

    def finish(self):
        other = 1 - self.o.core
        self.came(12, 1, self.q[1], core=other)
        for s in (1, 2):
            for m, step in enumerate(ARRIVE):
                self.came(10 + 3 * s + m, s, self.turn(s, step), core=other)

    def closed(self):
        for s, i in enumerate(self.q):
            for m, (step, half) in enumerate(((0, None), (0, None), (3, 0), (1, 1))):
                self.sent(4 * s + m, self.group(self.o.core, s, self.turn(s, step), half))
            for m, step in enumerate(ARRIVE if s else ()):
                self.sent(10 + 3 * s + m, self.group(self.o.core, s, self.turn(s, step)))
        self.sent(12, self.group(self.o.core, 1, self.q[1]))


class Scatter(Ring):
    SEMS = 16

    def __init__(self, place, color, width, terms, r0, r3, r2, r1, out, send, recv):
        super().__init__(place, color, width, send, recv)
        self.terms, self.r0, self.r, self.out = terms, r0, (r1, r2, r3), out

    def order(self, n):
        return (self.q[2] + (2, 1, 3, 0)[n]) % 4

    def exchange(self):
        for n in range(4):
            at = self.index(2, self.order(n))
            self.go(n, self.terms.at[(*at, 1 - self.o.core)], self.r0.at[at], self.o.partner)

    def group(self, s, j, half=None):
        ref = self.terms.at[(*self.index(s, j, half), self.o.core)]
        return ref.at[:, self.lanes(half)] if half is not None and s == 0 else ref

    def slot(self, s, n):
        if n >= 2:
            return self.r[s].at[n - 1]
        ref = self.r[s].at[0]
        if s == 0:
            return ref.at[:, self.lanes(n)]
        at = [EDGE] * s
        at[sorted(self.dims[:s]).index(self.dims[s - 1])] = pl.ds(2 * n, 2)
        return ref.at[tuple(at)]

    def add(self, held, others):
        lead = held.shape[:-2]
        if not lead:
            held[...] = sum((o[...].astype(F32) for o in others), held[...].astype(F32)).astype(BF16)
            return

        def one(p):
            at = (p,) if len(lead) == 1 else (p // lead[1], p % lead[1])
            held[at] = sum((o[at].astype(F32) for o in others), held[at].astype(F32)).astype(BF16)

        pl.loop(0, math.prod(lead), unroll=2 if len(lead) == 1 else 4)(one)

    def add_cores(self, n):
        at = self.index(2, self.order(n))
        self.landed(n, self.r0.at[at])
        self.add(self.terms.at[(*at, self.o.core)], [self.r0.at[at]])

    def first(self, s):
        i, right, left = self.sides(s)
        b = 4 + 4 * s
        self.go(b, self.group(s, self.turn(s, OVER), 0), self.slot(s, 0), right)
        self.go(b + 1, self.group(s, self.turn(s, OVER), 1), self.slot(s, 1), left)

    def second(self, s):
        i, right, left = self.sides(s)
        b = 4 + 4 * s
        for n, j, to in ((0, self.turn(s, AFTER), right), (1, self.turn(s, BEFORE), left)):
            self.landed(b + n, self.slot(s, n))
            self.add(self.group(s, j, n), [self.slot(s, n)])
            self.go(b + 2 + n, self.group(s, j), self.slot(s, 2 + n), to)

    def closed(self):
        for n in range(4):
            self.sent(n, self.terms.at[(*self.index(2, self.order(n)), self.o.core)])
        for s, i in enumerate(self.q):
            for m, (step, half) in enumerate(((2, 0), (2, 1), (1, None), (3, None))):
                self.sent(4 + 4 * s + m, self.group(s, self.turn(s, step), half))

    def third(self, s):
        b = 4 + 4 * s
        for n in (2, 3):
            self.landed(b + n, self.slot(s, n))
        held, others = self.group(s, self.q[s]), [self.slot(s, 2), self.slot(s, 3)]
        if s:
            self.add(held, others)
        else:
            self.out[...] = sum((o[...].astype(F32) for o in others), held[...].astype(F32)).astype(BF16)


def block_of(refs, matrix, start, width):
    return refs[matrix].at[start] if matrix == 2 else refs[matrix].at[:, pl.ds(start, width)]


def gathers_of(place, blocks, bufs, send, recv, local):
    return [Gather(place, c, w, block_of(blocks, m, at, w), bufs[n], send.at[n], recv.at[n], local.at[n])
            for n, (m, c, at, w) in enumerate(UNITS)]


def scatters_of(place, terms, r0s, r3s, r2s, r1s, outs, send, recv):
    return [Scatter(place, c, w, terms[n], r0s[n], r3s[n], r2s[n], r1s[n], block_of(outs, m, at, w), send.at[n], recv.at[n])
            for n, (m, c, at, w) in enumerate(UNITS)]


def unit_arrays(*lead):
    return [(*lead, 8, w) for _, _, _, w in UNITS]


def pick(rows, cols, back):
    r = lax.broadcasted_iota(jnp.int32, (rows, cols), 1 if back else 0)
    c = lax.broadcasted_iota(jnp.int32, (rows, cols), 0 if back else 1)
    return ((r == 7 * (c >> 3) + (c & 7)) & ((c & 7) < 7)).astype(F32).astype(BF16)


def dot(a, b, dims=((1,), (0,))):
    return lax.dot_general(a, b, (dims, ((), ())), preferred_element_type=F32)


def unpad(unit, buf, w, wide):
    matrix, _, start, width = UNITS[unit]
    for x in range(4):
        rows = buf[x].astype(F32).reshape(256, width).astype(BF16)
        w[pl.ds(224 * x, 224), pl.ds(start, width)] = dot(wide[...], rows).astype(BF16)


def unpad_down(bufs, w, tall):
    def some(x):
        for i in range(32):
            for r in range(3):
                tall[pl.ds(20 * i + 8 * r, 8), :] = bufs[r][x, i // 8, i // 2 % 4, i % 2].astype(F32)
        w[pl.ds(pl.multiple_of(640 * x, 128), 640), :] = tall[0:640, :].astype(BF16)
    pl.loop(0, 4)(some)

TILE, PART = 512, 1280
TILES, PARTS = TOKENS // TILE, FF // PART
SHORT = 256
HERE, VM = pl.BlockSpec(memory_space=pl.ANY), pl.BlockSpec(memory_space=pltpu.VMEM)


def normed(h):
    wide = h.astype(F32)
    scale = lax.rsqrt(jnp.mean(wide**2, -1, keepdims=True) + 1e-6)
    return wide, scale


def gather_semaphores():
    return [pltpu.SemaphoreType.DMA((9, Gather.SEMS)), pltpu.SemaphoreType.DMA((9, Gather.SEMS)), pltpu.SemaphoreType.DMA((9,))]


def up_kernel(x, *refs):
    blocks0, blocks1, (h1, a, gate_out, up_out), kept, bufs1, bufs0, w, refs = cut(refs, 3, 3, 4, 3, 9, 9, 3)
    tall, wide, acc, send0, recv0, local0, send1, recv1, local1, keep = refs
    i, j = pl.program_id(0), pl.program_id(1)
    step = i
    place = Place()
    ahead = gathers_of(place, blocks0, bufs0, send0, recv0, local0)
    later = gathers_of(place, blocks1, bufs1, send1, recv1, local1)
    keeps = [pltpu.make_async_copy(w[m], kept[m], keep.at[m]) for m in range(3)]

    @pl.when(step == 0)
    def _():
        for g in ahead + later:
            g.load()
        place.greet()
        for g in ahead:
            g.loaded()
            g.first(0)
        wide[...] = pick(224, 256, False)
        for s in range(3):
            for g in ahead:
                g.second(s)
            for g in ahead:
                g.third(s)
                if s < 2:
                    g.first(s + 1)
        for g in later:
            g.loaded()
            g.first(0)
        for n, g in enumerate(ahead):
            g.finish()
            if n < 6:
                unpad(n, bufs0[n], w[n // 3], wide)
        for g in later:
            g.second(0)
        unpad_down(bufs0[6:], w[2], tall)
        for k in keeps:
            k.start()
        for g in later:
            g.third(0)
            g.first(1)
        for g in ahead:
            g.closed()

    def second(s):
        for g in later:
            g.second(s)

    def third(s):
        for g in later:
            g.third(s)
            g.first(s + 1)

    pl.when(step == 1)(lambda: second(1))
    pl.when(step == 2)(lambda: third(1))
    pl.when(step == 5)(lambda: second(2))

    @pl.when(j == 0)
    def _():
        wide_h, scale = normed(x[...])
        a[...] = (wide_h * scale).astype(BF16)
        acc[...] = jnp.zeros_like(acc)

    lanes = pl.ds(0, FF)
    gate = dot(a[...], w[0][:, lanes])
    up = dot(a[...], w[1][:, lanes])
    gate_out[...] = gate
    up_out[...] = up
    act = (gate * jax.nn.sigmoid(gate) * up).astype(BF16)
    acc[...] += dot(act, w[2][lanes, :])

    @pl.when(j == 0)
    def _():
        h1[...] = (x[...].astype(F32) + acc[...].astype(BF16).astype(F32)).astype(BF16)

    @pl.when(step == TOKENS // SHORT - 1)
    def _():
        for g in later:
            g.third(2)
        for g in later:
            g.finish()
        for g in later:
            g.closed()
        for k in keeps:
            k.wait()


def params(collective=None):
    return pltpu.CompilerParams(collective_id=collective, has_side_effects=collective is not None, vmem_limit_bytes=67043328)


def tiled(tile, part):
    return pl.BlockSpec((tile, D), lambda i, j: (i, 0)), pl.BlockSpec((tile, part), lambda i, j: (i, j))


def like(shape, dtype=BF16):
    return jax.ShapeDtypeStruct(shape, dtype)


WEIGHTS = ((D, FF), (D, FF), (FF, D))
STATES, HIDDEN = (TOKENS, D), (TOKENS, FF)


def forward(x, blocks0, blocks1):
    rows, part = tiled(SHORT, FF)
    units = unit_arrays(*TORUS, 2)
    out = pl.pallas_call(
        up_kernel,
        grid=(TOKENS // SHORT, 1),
        out_shape=[like(STATES), like(STATES), like(HIDDEN, F32), like(HIDDEN, F32), *map(like, WEIGHTS), *map(like, units)],
        in_specs=[rows, *[HERE] * 6],
        out_specs=[rows, rows, part, part, *[HERE] * 12],
        scratch_shapes=[
            *[pltpu.VMEM(s, BF16) for s in (*units, *WEIGHTS)],
            pltpu.VMEM((648, D), F32), pltpu.VMEM((224, 256), BF16), pltpu.VMEM((SHORT, D), F32),
            *gather_semaphores(), *gather_semaphores(), pltpu.SemaphoreType.DMA((3,))],
        compiler_params=params(0),
    )(x, *blocks0, *blocks1)
    return cut(out, *[1] * 4, 3)


def hidden_back(gate, up, by_act):
    sig = jax.nn.sigmoid(gate)
    silu = gate * sig
    by_silu = by_act * up
    by_gate = by_silu * (sig + silu * (1 - sig))
    return (silu * up).astype(BF16), by_gate.astype(BF16), (by_act * silu).astype(BF16)


def norm_back(h, by_h, by_gate_a, by_up_a):
    by_a = (by_gate_a.astype(BF16).astype(F32) + by_up_a.astype(BF16).astype(F32)).astype(BF16).astype(F32)
    wide, scale = normed(h)
    by_scale = jnp.sum(by_a * wide, -1, keepdims=True)
    by_wide = by_a * scale - wide * (by_scale * scale**3 / D)
    return (by_h.astype(F32) + by_wide.astype(BF16).astype(F32)).astype(BF16)


BACK = ((1,), (1,))


def back_part(h, by_h, gate, up, w, lanes, outs, by_in, accs, last):
    by_act = dot(by_h[...], w[2][lanes, :], BACK).astype(BF16).astype(F32)
    for out, value in zip(outs, hidden_back(gate, up, by_act)):
        out[...] = value
    for k, acc in enumerate(accs):
        acc[...] += dot(outs[k + 1][...], w[k][:, lanes], BACK)

    @pl.when(last)
    def _():
        by_in[...] = norm_back(h[...], by_h[...], accs[0][...], accs[1][...])


def top_kernel(*refs):
    bufs, (h, by_h, a), outs, (by_in,), w, accs, (stage, tall, wide, fetch) = cut(refs, 9, 3, 3, 1, 3, 2)
    i, j = pl.program_id(0), pl.program_id(1)

    @pl.when((i == 0) & (j == 0))
    def _():
        held = [stage.at[n % 3, :, :, :, :, :, pl.ds(0, UNITS[n][3])] for n in range(9)]
        copies = [pltpu.make_async_copy(bufs[n], held[n], fetch.at[n % 3]) for n in range(9)]
        for n in range(3):
            copies[n].start()
        wide[...] = pick(224, 256, False)
        for n in range(6):
            copies[n].wait()
            unpad(n, held[n], w[n // 3], wide)
            copies[n + 3].start()
        for n in range(6, 9):
            copies[n].wait()
        unpad_down(held[6:], w[2], tall)

    @pl.when(j == 0)
    def _():
        wide_h, scale = normed(h[...])
        a[...] = (wide_h * scale).astype(BF16)
        for acc in accs:
            acc[...] = jnp.zeros_like(acc)

    lanes = pl.ds(0, FF)
    gate = dot(a[...], w[0][:, lanes])
    up = dot(a[...], w[1][:, lanes])
    back_part(h, by_h, gate, up, w, lanes, outs, by_in, accs, j == 0)


def top(h, by_h, bufs):
    rows, part = tiled(SHORT, FF)
    return pl.pallas_call(
        top_kernel,
        grid=(TOKENS // SHORT, 1),
        out_shape=[like(STATES), *[like(HIDDEN)] * 3, like(STATES)],
        in_specs=[*[HERE] * 9, rows, rows],
        out_specs=[rows, part, part, part, rows],
        scratch_shapes=[*[pltpu.VMEM(s, BF16) for s in WEIGHTS], *[pltpu.VMEM((SHORT, D), F32)] * 2,
                        pltpu.VMEM((3, 4, 4, 4, 2, 8, 1024), BF16), pltpu.VMEM((648, D), F32), pltpu.VMEM((224, 256), BF16),
                        pltpu.SemaphoreType.DMA((3,))],
        compiler_params=params(),
    )(*bufs, h, by_h)


COLS = 256


def sum_kernel(below, *refs):
    (a, by_h, act, by_gate, by_up), came, outs, gone, refs = cut(refs, 5, 7 * below, 3, 4 * below)
    terms, r0s, r3s, r2s, r1s, refs = cut(refs, *[len(UNITS)] * 5)
    back, send, recv, fetch, fetch_wide, whole = refs
    def all_units():
        return scatters_of(Place(), terms, r0s, r3s, r2s, r1s, outs, send, recv)

    units = all_units()

    def cores(some):
        for n in range(4):
            for k in some:
                k.add_cores(n)
            if not n:
                for k in some:
                    k.first(2)

    def steps(plan, units=units):
        for what, which in zip(plan[::2], plan[1::2]):
            some = [k for k, unit in zip(units, "ggguuuddd") if unit == which]
            if what == "c":
                cores(some)
            for k in some:
                if what == "b":
                    k.second(2)
                elif what == "f":
                    k.third(2)
                    k.first(1)
                elif what == "h":
                    k.second(1)
                elif what == "k":
                    k.third(1)
                    k.first(0)
                elif what == "m":
                    k.second(0)
                elif what == "p":
                    k.third(0)

    units[0].o.greet()
    back[...] = pick(256, 224, True)

    def make_all(side, tall, cols, made):
        def wide_copy(x):
            return pltpu.make_async_copy(act.at[:, pl.ds(pl.multiple_of(640 * x, 128), 640)], cols.at[x % 2], fetch_wide.at[x % 2])

        def copy(src, t):
            return pltpu.make_async_copy(
                src.at[:, pl.ds(pl.multiple_of(COLS * t, COLS), COLS)], cols.at[t % 2, :, pl.ds(0, COLS)], fetch.at[t % 2])

        states = pltpu.make_async_copy(by_h, side, whole)
        states.start()
        wide_copy(0).start()
        states.wait()
        tall[640:648, :] = jnp.zeros((8, D), F32)

        def down(x):
            wide_copy(x).wait()
            pl.when(x < 3)(lambda: wide_copy(x + 1).start())
            tall[0:640, :] = dot(cols[x % 2], side[...], ACROSS)
            for i in range(32):
                for r in range(3):
                    terms[6 + r][x, i // 8, i // 2 % 4, i % 2] = tall[pl.ds(20 * i + 8 * r, 8), :].astype(BF16)

        pl.loop(0, 4)(down)
        states = pltpu.make_async_copy(a, side, whole)
        states.start()
        copy(by_gate, 0).start()
        for k in units[6:]:
            k.exchange()
        states.wait()

        for unit, then in enumerate(("cd", "", "bdcg", "fd", "hdbg", "kdfg")):
            matrix, _, start, width = UNITS[unit]
            src, term = (by_gate, by_up)[matrix], terms[unit]

            def one(n):
                t = start // COLS + n
                copy(src, t).wait()
                pl.when(t < FF // COLS - 1)(lambda: copy(src, t + 1).start())
                lanes = pl.ds(pl.multiple_of(n * COLS, COLS), COLS)
                made[:, lanes] = dot(side[...], cols[t % 2, :, 0:COLS], ACROSS).astype(BF16)

            pl.loop(0, width // COLS)(one)
            for x in range(4):
                term[x] = dot(back[...], made[224 * x:224 * (x + 1), 0:width]).reshape(4, 4, 2, 8, width).astype(BF16)
            if unit == 2:
                copy(by_up, 0).start()
            units[unit].exchange()
            steps(then)

    pl.run_scoped(make_all, pltpu.VMEM(STATES, BF16), pltpu.VMEM((648, D), F32), pltpu.VMEM((2, TOKENS, 640), BF16),
                  pltpu.VMEM((D, 1024), BF16))

    if not below:
        steps("mdcuhgpdkgbumgfupghukumupu")
    else:
        def lower(*refs):
            w, accs = cut(refs, 3)
            loads = [pltpu.make_async_copy(came[k + 4], w[k], fetch.at[0] if not k else fetch_wide.at[k - 1]) for k in range(3)]
            for load in loads:
                load.start()
            steps("mdcu")
            for load in loads:
                load.wait()
            rows, part = tiled(SHORT, PART)

            def body(h, by_next, gate, up, act_out, by_gate_out, by_up_out, by_in):
                i, j = pl.program_id(0), pl.program_id(1)
                for n, plan in enumerate(("hgpd", "kg", "bu", "mg", "pg", "fu", "", "hu", "", "ku", "mu", "", "pu")):
                    if plan:
                        pl.when(i * PARTS + j == n)(lambda: steps(plan, all_units()))

                @pl.when(j == 0)
                def _():
                    for acc in accs:
                        acc[...] = jnp.zeros_like(acc)

                lanes = pl.ds(pl.multiple_of(j * PART, PART), PART)
                back_part(h, by_next, gate[...], up[...], w, lanes, (act_out, by_gate_out, by_up_out), by_in, accs, j == PARTS - 1)

            pltpu.emit_pipeline(
                body, grid=(TOKENS // SHORT, PARTS), in_specs=[rows, rows, part, part], out_specs=[part, part, part, rows])(*came[:4], *gone)

        pl.run_scoped(lower, *[pltpu.VMEM(s, BF16) for s in WEIGHTS], *[pltpu.VMEM((SHORT, D), F32)] * 2)
    for k in units:
        k.closed()


ACROSS = ((0,), (0,))


def summed(a, by_h, act, by_gate, by_up, below=()):
    arrays = lambda *lead: [pltpu.VMEM(s, BF16) for s in unit_arrays(*lead)]
    more = [*[like(HIDDEN)] * 3, like(STATES)] if below else []
    g, u, d, *gone = pl.pallas_call(
        lambda *refs: sum_kernel(bool(below), *refs),
        out_shape=[like((8, FF)), like((8, FF)), like((3, 8, D)), *more],
        in_specs=[HERE] * (5 + len(below)),
        out_specs=[VM] * 3 + [HERE] * len(more),
        scratch_shapes=[
            *arrays(*TORUS, 2), *arrays(*TORUS), *arrays(3, 4, 4), *arrays(3, 4), *arrays(3),
            pltpu.VMEM((256, 224), BF16),
            pltpu.SemaphoreType.DMA((9, Scatter.SEMS)), pltpu.SemaphoreType.DMA((9, Scatter.SEMS)),
            pltpu.SemaphoreType.DMA((2,)), pltpu.SemaphoreType.DMA((2,)), pltpu.SemaphoreType.DMA],
        compiler_params=params(1 + len(below)),
    )(a, by_h, act, by_gate, by_up, *below)
    return (g[:7], u[:7], d.reshape(24, D)[:20]), gone


def pad_blocks(g, u, d):
    return jnp.pad(g, ((0, 1), (0, 0))), jnp.pad(u, ((0, 1), (0, 0))), jnp.pad(d, ((0, 4), (0, 0))).reshape(3, 8, D)


def solution(mesh):
    def step(x, dy, w_gate, w_up, w_down):
        x, dy = x[0], dy[0]
        blocks = [pad_blocks(w_gate[n], w_up[n], w_down[n]) for n in range(2)]
        (h1,), (a0,), (gate,), (up,), w0, bufs1 = forward(x, *blocks)
        a1, act1, by_gate1, by_up1, by_h1 = top(h1, dy, bufs1)
        sums1, (*parts0, by_x) = summed(a1, dy, act1, by_gate1, by_up1, below=(x, by_h1, gate, up, *w0))
        sums0, _ = summed(a0, by_h1, *parts0)
        return (by_x[None], *(jnp.stack([sums0[k], sums1[k]]) for k in range(3)))

    rows = P(("rep", "dp"))
    weights = [P(None, "dp")] * 3
    return jax.shard_map(step, mesh=mesh, in_specs=(rows, rows, *weights), out_specs=(rows, *weights), check_vma=False)
```
